8 devices in a mesh: dp: 1 (over z), tp: 2 (over y), cp: 4 (over x, core).
Axes of the slice: x: 2, y: 2, z: 1, core: 2. Of those that a mesh axis runs over, the one named last changes fastest.
Arguments:
- hidden: bfloat16 [2048, 4096], P(('dp', 'cp', 'tp'))
- positions: int32 [2048], P(('dp', 'cp', 'tp'))
- doc_ids: int32 [2048], P(('dp', 'cp', 'tp'))
- attn_gain: bfloat16 [4096], replicated
- mlp_gain: bfloat16 [4096], replicated
- w_query: bfloat16 [4096, 4096], P(None, 'tp')
- w_key: bfloat16 [4096, 1024], P(None, 'tp')
- w_value: bfloat16 [4096, 1024], P(None, 'tp')
- w_out: bfloat16 [4096, 4096], P('tp')
- w_gate: bfloat16 [4096, 14336], P(None, 'tp')
- w_up: bfloat16 [4096, 14336], P(None, 'tp')
- w_down: bfloat16 [14336, 4096], P('tp')
Outputs:
- output: bfloat16 [2048, 4096], P(('dp', 'cp', 'tp'))
All inputs are finite; a program needn't handle non-finite values.
Results may differ from the reference program's by a relative error of at most 0.0119203.
Values are sent between devices in bfloat16 or wider.
A program may use at most 1 GiB of HBM per device.

```python
import math
import jax
import jax.numpy as jnp
from jax import lax

ROWS_DEV = 256
SHARDS = 8
MODEL_DIM = 4096
Q_HEADS = 32
KV_HEADS = 8
HEAD_DIM = 128
FFN_DIM = 14336
NUM_DOCS = 4
TOKENS = ROWS_DEV * SHARDS
Q_BLOCK = math.gcd(TOKENS, 32)
SCORE_VAR = math.log(TOKENS / 16.0)
ROPE_BASE = 500000.0
NORM_EPS = 1e-5
NEG_BIG = -1e30


def arrange(values):
    pieces = values.reshape(2 * SHARDS, TOKENS // (2 * SHARDS))
    return jnp.stack([pieces[:SHARDS], pieces[SHARDS:][::-1]], axis=1).reshape(TOKENS)


def doc_layout(doc_key):
    cut_points = jnp.sort(jax.random.permutation(doc_key, TOKENS - 1)[: NUM_DOCS - 1] + 1).astype(jnp.int32)
    logical = jnp.arange(TOKENS, dtype=jnp.int32)
    doc_logical = jnp.sum((logical[:, None] >= cut_points[None, :]).astype(jnp.int32), axis=1)
    starts = jnp.concatenate([jnp.zeros((1,), jnp.int32), cut_points])
    pos_logical = logical - starts[doc_logical]
    return arrange(pos_logical), arrange(doc_logical)


def normal_weight(weight_key, arr_shape, std_scale):
    return (jax.random.normal(weight_key, arr_shape, jnp.float32) * std_scale).astype(jnp.bfloat16)


def setup_inputs(seed: int = 0, part: int = 0) -> dict:
    base_key = jax.random.key(seed)
    part_key = jax.random.fold_in(base_key, part)
    hidden_key, doc_key = jax.random.split(part_key)
    weight_keys = jax.random.split(base_key, 9)
    positions, doc_ids = doc_layout(doc_key)
    q_cols = Q_HEADS * HEAD_DIM
    kv_cols = KV_HEADS * HEAD_DIM
    qk_scale = SCORE_VAR ** 0.25 * MODEL_DIM ** -0.5
    return {
        'hidden': normal_weight(hidden_key, (TOKENS, MODEL_DIM), 1.0),
        'positions': positions,
        'doc_ids': doc_ids,
        'attn_gain': (1.0 + 0.25 * jax.random.normal(weight_keys[0], (MODEL_DIM,), jnp.float32)).astype(jnp.bfloat16),
        'mlp_gain': (1.0 + 0.25 * jax.random.normal(weight_keys[1], (MODEL_DIM,), jnp.float32)).astype(jnp.bfloat16),
        'w_query': normal_weight(weight_keys[2], (MODEL_DIM, q_cols), qk_scale),
        'w_key': normal_weight(weight_keys[3], (MODEL_DIM, kv_cols), qk_scale),
        'w_value': normal_weight(weight_keys[4], (MODEL_DIM, kv_cols), MODEL_DIM ** -0.5),
        'w_out': normal_weight(weight_keys[5], (q_cols, MODEL_DIM), q_cols ** -0.5),
        'w_gate': normal_weight(weight_keys[6], (MODEL_DIM, FFN_DIM), MODEL_DIM ** -0.5),
        'w_up': normal_weight(weight_keys[7], (MODEL_DIM, FFN_DIM), MODEL_DIM ** -0.5),
        'w_down': normal_weight(weight_keys[8], (FFN_DIM, MODEL_DIM), FFN_DIM ** -0.5),
    }


def rms_norm(values, gain_vec):
    wide_vals = values.astype(jnp.float32)
    inv_rms = lax.rsqrt(jnp.mean(wide_vals * wide_vals, axis=-1, keepdims=True) + NORM_EPS)
    return (wide_vals * inv_rms * gain_vec.astype(jnp.float32)).astype(jnp.bfloat16)


def rotary(vectors, positions):
    half_dim = vectors.shape[-1] // 2
    inv_freq = ROPE_BASE ** (-jnp.arange(half_dim, dtype=jnp.float32) * (2.0 / vectors.shape[-1]))
    angles = positions.astype(jnp.float32)[:, None] * inv_freq[None, :]
    cos_ang = jnp.cos(angles)[:, None, :]
    sin_ang = jnp.sin(angles)[:, None, :]
    first_half = vectors[..., :half_dim]
    second_half = vectors[..., half_dim:]
    return jnp.concatenate([first_half * cos_ang - second_half * sin_ang, second_half * cos_ang + first_half * sin_ang], axis=-1)


def reference(hidden, positions, doc_ids, attn_gain, mlp_gain, w_query, w_key, w_value, w_out, w_gate, w_up, w_down):
    group_size = Q_HEADS // KV_HEADS
    normed = rms_norm(hidden, attn_gain)
    queries = rotary(jnp.dot(normed, w_query, preferred_element_type=jnp.float32).reshape(TOKENS, Q_HEADS, HEAD_DIM), positions).astype(jnp.bfloat16)
    keys_rot = rotary(jnp.dot(normed, w_key, preferred_element_type=jnp.float32).reshape(TOKENS, KV_HEADS, HEAD_DIM), positions).astype(jnp.bfloat16)
    values_all = jnp.dot(normed, w_value, preferred_element_type=jnp.float32).astype(jnp.bfloat16).reshape(TOKENS, KV_HEADS, HEAD_DIM)
    keys_wide = keys_rot.astype(jnp.float32)
    values_wide = values_all.astype(jnp.float32)
    n_blocks = TOKENS // Q_BLOCK
    q_blocks = queries.reshape(n_blocks, Q_BLOCK, KV_HEADS, group_size, HEAD_DIM)
    pos_blocks = positions.reshape(n_blocks, Q_BLOCK)
    doc_blocks = doc_ids.reshape(n_blocks, Q_BLOCK)

    def attend(block_in):
        q_blk, query_pos, query_doc = block_in
        scores = jnp.einsum('qhgd,khd->hgqk', q_blk.astype(jnp.float32), keys_wide) * (HEAD_DIM ** -0.5)
        visible = (query_doc[:, None] == doc_ids[None, :]) & (positions[None, :] <= query_pos[:, None])
        scores = jnp.where(visible, scores, NEG_BIG)
        row_max = jnp.max(scores, axis=-1, keepdims=True)
        weights = jnp.where(visible, jnp.exp(scores - row_max), 0.0)
        row_sum = jnp.sum(weights, axis=-1, keepdims=True)
        block_mix = jnp.einsum('hgqk,khd->hgqd', weights.astype(jnp.bfloat16).astype(jnp.float32), values_wide) / row_sum
        return jnp.transpose(block_mix, (2, 0, 1, 3)).astype(jnp.bfloat16)

    attn_mix = lax.map(attend, (q_blocks, pos_blocks, doc_blocks)).reshape(TOKENS, Q_HEADS * HEAD_DIM)
    attn_out = jnp.dot(attn_mix, w_out, preferred_element_type=jnp.float32)
    residual = (hidden.astype(jnp.float32) + attn_out).astype(jnp.bfloat16)
    normed_mlp = rms_norm(residual, mlp_gain)
    gate_val = jnp.dot(normed_mlp, w_gate, preferred_element_type=jnp.float32)
    up_val = jnp.dot(normed_mlp, w_up, preferred_element_type=jnp.float32)
    gated = (jax.nn.silu(gate_val) * up_val).astype(jnp.bfloat16)
    down_val = jnp.dot(gated, w_down, preferred_element_type=jnp.float32)
    return (residual.astype(jnp.float32) + down_val).astype(jnp.bfloat16)
```

```python
import functools

import jax
import jax.numpy as jnp
from jax import lax
from jax.experimental import pallas as pl
from jax.experimental.pallas import tpu as pltpu
from jax.sharding import PartitionSpec as P

HEAD = 128
ROPE_BASE = 500000.0
EPS = 1e-5
PIECE = 128
KEYS = 256
SCALE = (HEAD ** -0.5) * 1.4426950408889634
NEG = -1e30
F32 = jnp.float32
BF16 = jnp.bfloat16
ANY = pl.BlockSpec(memory_space=pl.ANY)
VM = pl.BlockSpec(memory_space=pltpu.VMEM)
VMEM_BIG = 67_000_000


def rope_tables(positions):
    lane = jnp.arange(HEAD, dtype=jnp.int32)
    half = (lane % (HEAD // 2)).astype(F32)
    inv = ROPE_BASE ** (-half * (2.0 / HEAD))
    ang = positions.astype(F32)[:, None] * inv[None, :]
    sign = jnp.where(lane < HEAD // 2, -1.0, 1.0).astype(F32)
    pos = jnp.broadcast_to(positions[:, None], ang.shape)
    return jnp.cos(ang), jnp.sin(ang) * sign[None, :], pos


def rope_store(u, cos, sin, out_ref):
    for h in range(u.shape[1] // HEAD):
        v = u[:, h * HEAD:(h + 1) * HEAD]
        r = v * cos + pltpu.roll(v, HEAD // 2, 1) * sin
        out_ref[:, h * HEAD:(h + 1) * HEAD] = r.astype(BF16)


def norm_rows(load, gain, a_ref, rows):
    @pl.loop(0, rows // 16, unroll=2)
    def _(i):
        sl = pl.ds(pl.multiple_of(i * 16, 16), 16)
        v = load(sl)
        r = lax.rsqrt(jnp.mean(v * v, axis=-1, keepdims=True) + EPS)
        a_ref[sl, :] = (v * r * gain).astype(BF16)


def kv_kernel(x_ref, g_ref, cos_ref, sin_ref, wk_ref, wv_ref, after_ref, kv_ref, a_ref, x_s, wk_s, wv_s, sem):
    rows, kvw = x_s.shape[0], wk_s.shape[1]
    cx = pltpu.make_async_copy(x_ref.at[pl.ds(0, rows)], x_s, sem.at[0])
    ck = pltpu.make_async_copy(wk_ref, wk_s, sem.at[1])
    cv = pltpu.make_async_copy(wv_ref, wv_s, sem.at[2])
    for cp in (cx, ck, cv):
        cp.start()
    cx.wait()
    norm_rows(lambda sl: x_s[sl, :].astype(F32), g_ref[...].astype(F32), a_ref, rows)
    a = a_ref[...]
    ck.wait()
    u = jnp.dot(a, wk_s[...], preferred_element_type=F32)
    rope_store(u, cos_ref[...], sin_ref[...], kv_ref)
    cv.wait()
    kv_ref[:, kvw:] = jnp.dot(a, wv_s[...], preferred_element_type=F32).astype(BF16)


def kv_call(x, gain, cos, sin, wk, wv, after):
    rows, d = x.shape
    kvw = wk.shape[1]
    return pl.pallas_call(
        kv_kernel,
        in_specs=[ANY, VM, VM, VM, ANY, ANY, ANY],
        out_specs=[VM, VM],
        out_shape=[jax.ShapeDtypeStruct((rows, 2 * kvw), BF16), jax.ShapeDtypeStruct((rows, d), BF16)],
        scratch_shapes=[
            pltpu.VMEM((rows, d), BF16),
            pltpu.VMEM((d, kvw), BF16),
            pltpu.VMEM((d, kvw), BF16),
            pltpu.SemaphoreType.DMA((3,)),
        ],
        compiler_params=pltpu.CompilerParams(vmem_limit_bytes=VMEM_BIG),
        cost_estimate=pl.CostEstimate(flops=2 * rows * d * 2 * kvw, bytes_accessed=4 * d * kvw + 4 * rows * d, transcendentals=0),
        name="kv",
    )(x, gain, cos, sin, wk, wv, after)


def q_kernel(a_ref, cos_ref, sin_ref, wq_ref, after_ref, q_ref):
    u = jnp.dot(a_ref[...], wq_ref[...], preferred_element_type=F32)
    rope_store(u, cos_ref[...], sin_ref[...], q_ref)


def q_call(a, cos, sin, wq, after):
    rows, d = a.shape
    n = wq.shape[1]
    t = 512
    const = lambda j: (0, 0)
    return pl.pallas_call(
        q_kernel,
        grid=(n // t,),
        in_specs=[
            pl.BlockSpec((rows, d), const),
            pl.BlockSpec((rows, HEAD), const),
            pl.BlockSpec((rows, HEAD), const),
            pl.BlockSpec((d, t), lambda j: (0, j)),
            ANY,
        ],
        out_specs=pl.BlockSpec((rows, t), lambda j: (0, j)),
        out_shape=jax.ShapeDtypeStruct((rows, n), BF16),
        compiler_params=pltpu.CompilerParams(vmem_limit_bytes=VMEM_BIG),
        cost_estimate=pl.CostEstimate(flops=2 * rows * d * n, bytes_accessed=2 * d * n + 2 * rows * d, transcendentals=0),
        name="q",
    )(a, cos, sin, wq, after)


def attn_kernel(n_cp, late, entries, first_ref, pos_ref, *refs):
    per = 3 if late else 2
    n_q = len(entries)
    q_refs, wo_ref, chunks = refs[:n_q], refs[n_q], refs[n_q + 2:n_q + 2 + per * n_cp]
    refs = refs[n_q + 2 + per * n_cp:]
    m_refs = refs[:n_q]
    q_s, kv_s, s_s, mx_s, tot_s, acc_s, o_s, wo_s, qsem, sem, wsem = refs[n_q:]
    c, t = lax.axis_index("cp"), lax.axis_index("tp")
    n_piece = 4 * n_cp
    kvw = kv_s.shape[1] // 2
    heads = q_s.shape[1] // HEAD
    n_kv = kvw // HEAD
    grp = heads // n_kv
    rows = grp * PIECE

    def rows_of(piece):
        return pl.ds(pl.multiple_of(piece * PIECE, PIECE), PIECE)

    qcopies = []
    for w, ref in enumerate(q_refs):
        src = ref if ref.shape[0] == PIECE else ref.at[pl.ds(PIECE * entries[w][1], PIECE)]
        qcopies.append(pltpu.make_async_copy(src, q_s.at[pl.ds(w * PIECE, PIECE)], qsem.at[w]))
    copies = []
    for i in range(n_cp):
        ci = lax.bitwise_xor(c, i)
        mine, other = 2 * ci + t, 2 * ci + 1 - t
        own = chunks[per * i]
        pairs = [(own.at[pl.ds(0, PIECE)], mine), (chunks[per * i + 1], other)]
        if late:
            pairs += [(own.at[pl.ds(PIECE, PIECE)], n_piece - 1 - mine), (chunks[per * i + 2], n_piece - 1 - other)]
        for src, piece in pairs:
            copies.append(pltpu.make_async_copy(src, kv_s.at[rows_of(piece)], sem.at[len(copies)]))
    wide = wo_ref.shape[1] // 4
    wcopies = [pltpu.make_async_copy(wo_ref.at[:, pl.ds(i * wide, wide)], wo_s.at[:, pl.ds(i * wide, wide)], wsem.at[i]) for i in range(4)]
    for cp in qcopies + copies + wcopies:
        cp.start()
    for cp in qcopies + copies:
        cp.wait()

    lane = lax.broadcasted_iota(jnp.int32, (PIECE, KEYS), 1)
    row = lax.broadcasted_iota(jnp.int32, (PIECE, KEYS), 0)
    for w, (partner, second) in enumerate(entries):
        me = 2 * c + (1 - t if partner else t)
        q_ref = q_s.at[pl.ds(w * PIECE, PIECE)]
        pos = jnp.concatenate([pos_ref[PIECE * second:PIECE * (second + 1), :]] * (KEYS // HEAD), axis=1)
        mx_s[...] = jnp.full(mx_s.shape, NEG, F32)
        tot_s[...] = jnp.zeros(tot_s.shape, F32)
        acc_s[...] = jnp.zeros(acc_s.shape, F32)
        base = (n_piece - 1 - me if second else me) * PIECE
        last = row + base
        start = last - pos
        k0 = (base - first_ref[second]) // KEYS
        k1 = (base + PIECE - 1) // KEYS + 1

        @pl.loop(k0, k1)
        def _(kb):
            off = pl.multiple_of(kb * KEYS, KEYS)
            j = lane + off
            vis = (j >= start) & (j <= last)
            for g in range(n_kv):
                k = kv_s[pl.ds(off, KEYS), g * HEAD:(g + 1) * HEAD]
                qs = jnp.concatenate(
                    [q_ref[:, (g * grp + h) * HEAD:(g * grp + h + 1) * HEAD] for h in range(grp)], axis=0)
                s = lax.dot_general(qs, k, (((1,), (1,)), ((), ())), preferred_element_type=F32)
                for h in range(grp):
                    sh = jnp.where(vis, s[h * PIECE:(h + 1) * PIECE], NEG)
                    r = slice(g * rows + h * PIECE, g * rows + (h + 1) * PIECE)
                    s_s[kb, r, :] = sh
                    mx_s[r, :] = jnp.maximum(mx_s[r, :], jnp.maximum(sh[:, :HEAD], sh[:, HEAD:]))

        for g in range(n_kv):
            r = slice(g * rows, (g + 1) * rows)
            mx_s[r, :] = jnp.broadcast_to(jnp.max(mx_s[r, :], axis=-1, keepdims=True) * SCALE, (rows, HEAD))

        @pl.loop(k0, k1)
        def _(kb):
            off = pl.multiple_of(kb * KEYS, KEYS)
            for g in range(n_kv):
                r = slice(g * rows, (g + 1) * rows)
                v = kv_s[pl.ds(off, KEYS), kvw + g * HEAD:kvw + (g + 1) * HEAD]
                m = mx_s[r, :]
                e0 = jnp.exp2(s_s[kb, r, :HEAD] * SCALE - m)
                e1 = jnp.exp2(s_s[kb, r, HEAD:] * SCALE - m)
                tot_s[r, :] += e0 + e1
                e = jnp.concatenate([e0.astype(BF16), e1.astype(BF16)], axis=1)
                acc_s[r, :] += jnp.dot(e, v, preferred_element_type=F32)

        for g in range(n_kv):
            for h in range(grp):
                r = slice(g * rows + h * PIECE, g * rows + (h + 1) * PIECE)
                den = jnp.sum(tot_s[r, :], axis=-1, keepdims=True)
                o_s[w * PIECE:(w + 1) * PIECE, (g * grp + h) * HEAD:(g * grp + h + 1) * HEAD] = (acc_s[r, :] / den).astype(BF16)

    o = o_s[...]
    for i, cp in enumerate(wcopies):
        cp.wait()
        cs = slice(i * wide, (i + 1) * wide)
        u = jnp.dot(o, wo_s[:, cs], preferred_element_type=F32).astype(BF16)
        for w in range(n_q):
            m_refs[w][:, cs] = u[w * PIECE:(w + 1) * PIECE]


def attn_call(n_cp, late, entries, first, pos, qs, wo, after, chunks, name):
    n, d = wo.shape
    kv2 = chunks[0].shape[1]
    grp = n // (kv2 // 2)
    n_kv = kv2 // 2 // HEAD
    n_keys = (4 if late else 2) * n_cp * PIECE
    n_q = len(entries)
    return pl.pallas_call(
        functools.partial(attn_kernel, n_cp, late, entries),
        in_specs=[pl.BlockSpec(memory_space=pltpu.SMEM), VM] + [ANY] * (n_q + 2 + len(chunks)),
        out_specs=[VM] * n_q,
        out_shape=[jax.ShapeDtypeStruct((PIECE, d), BF16)] * n_q,
        scratch_shapes=[
            pltpu.VMEM((n_q * PIECE, n), BF16),
            pltpu.VMEM((n_keys, kv2), BF16),
            pltpu.VMEM((n_keys // KEYS, n_kv * grp * PIECE, KEYS), F32),
            pltpu.VMEM((n_kv * grp * PIECE, HEAD), F32),
            pltpu.VMEM((n_kv * grp * PIECE, HEAD), F32),
            pltpu.VMEM((n_kv * grp * PIECE, HEAD), F32),
            pltpu.VMEM((n_q * PIECE, n), BF16),
            pltpu.VMEM((n, d), BF16),
            pltpu.SemaphoreType.DMA((n_q,)),
            pltpu.SemaphoreType.DMA((4 * n_cp,)),
            pltpu.SemaphoreType.DMA((4,)),
        ],
        compiler_params=pltpu.CompilerParams(vmem_limit_bytes=VMEM_BIG),
        cost_estimate=pl.CostEstimate(flops=2 * n_q * PIECE * n * (n_keys + d), bytes_accessed=2 * n_keys * kv2 + 2 * n * d, transcendentals=0),
        name=name,
    )(first, pos, *qs, wo, after, *chunks)


def add_kernel(h_ref, d_ref, r_ref, o_ref):
    o_ref[...] = (h_ref[...].astype(F32) + (d_ref[...].astype(F32) + r_ref[...].astype(F32))).astype(BF16)


def add_call(h, d, r):
    rows, cols = h.shape
    blk = pl.BlockSpec((rows // 4, cols), lambda i: (i, 0))
    return pl.pallas_call(
        add_kernel,
        grid=(4,),
        in_specs=[blk] * 3,
        out_specs=blk,
        out_shape=jax.ShapeDtypeStruct((rows, cols), BF16),
        compiler_params=pltpu.CompilerParams(vmem_limit_bytes=VMEM_BIG),
        cost_estimate=pl.CostEstimate(flops=2 * rows * cols, bytes_accessed=8 * rows * cols, transcendentals=0),
        name="add",
    )(h, d, r)


HID = 512


def mlp_kernel(xa_ref, xb_ref, ma_ref, mb_ref, ra_ref, rb_ref, g_ref, w1_ref, w3_ref, w2_ref, after_ref,
               d_ref, h_ref, x_s, m_s, r_s, b_s, acc_s, w1_s, w3_s, w2_s, xsem, sem1, sem3, sem2):
    steps = w1_ref.shape[1] // HID

    def up_copies(j, slot):
        cs = pl.ds(pl.multiple_of(j * HID, HID), HID)
        return (pltpu.make_async_copy(w1_ref.at[:, cs], w1_s.at[slot], sem1.at[slot]),
                pltpu.make_async_copy(w3_ref.at[:, cs], w3_s.at[slot], sem3.at[slot]))

    def down_copy(j, slot):
        cs = pl.ds(pl.multiple_of(j * HID, HID), HID)
        return pltpu.make_async_copy(w2_ref.at[cs], w2_s.at[slot], sem2.at[slot])

    loads = []
    for refs, dst in (((xa_ref, xb_ref), x_s), ((ma_ref, mb_ref), m_s), ((ra_ref, rb_ref), r_s)):
        for w, ref in enumerate(refs):
            loads.append(pltpu.make_async_copy(ref, dst.at[pl.ds(w * PIECE, PIECE)], xsem.at[len(loads)]))
    for cp in loads:
        cp.start()
    for j in range(2):
        for cp in up_copies(j, j):
            cp.start()
        down_copy(j, j).start()
    acc_s[...] = jnp.zeros_like(acc_s)
    for cp in loads:
        cp.wait()
    gain = g_ref[...].astype(F32)

    @pl.loop(0, 2 * PIECE // 16, unroll=2)
    def _(i):
        sl = pl.ds(pl.multiple_of(i * 16, 16), 16)
        h = x_s[sl, :].astype(F32) + (m_s[sl, :].astype(F32) + r_s[sl, :].astype(F32))
        hb = h.astype(BF16)
        h_ref[sl, :] = hb
        v = hb.astype(F32)
        r = lax.rsqrt(jnp.mean(v * v, axis=-1, keepdims=True) + EPS)
        b_s[sl, :] = (v * r * gain).astype(BF16)

    def step(j, ahead):
        slot = j % 2
        for cp in up_copies(j, slot):
            cp.wait()
        b = b_s[...]
        gate = jnp.dot(b, w1_s[slot], preferred_element_type=F32)
        up = jnp.dot(b, w3_s[slot], preferred_element_type=F32)
        if ahead:
            for cp in up_copies(j + 2, slot):
                cp.start()
        hid = (gate * jax.nn.sigmoid(gate) * up).astype(BF16)
        down_copy(j, slot).wait()
        acc_s[...] += jnp.dot(hid, w2_s[slot], preferred_element_type=F32)
        if ahead:
            down_copy(j + 2, slot).start()

    @pl.loop(0, steps - 2)
    def _(j):
        step(j, True)

    @pl.loop(steps - 2, steps)
    def _(j):
        step(j, False)

    d_ref[...] = acc_s[...].astype(BF16)


def mlp_call(x, mine, got, gain, w1, w3, w2, after, name):
    rows, d = 2 * PIECE, w1.shape[0]
    f = w1.shape[1]
    vm = pl.BlockSpec(memory_space=pltpu.VMEM)
    return pl.pallas_call(
        mlp_kernel,
        in_specs=[ANY] * 6 + [vm] + [ANY] * 4,
        out_specs=[vm, vm],
        out_shape=[jax.ShapeDtypeStruct((rows, d), BF16)] * 2,
        scratch_shapes=[pltpu.VMEM((rows, d), BF16)] * 4 + [
            pltpu.VMEM((rows, d), F32),
            pltpu.VMEM((2, d, HID), BF16),
            pltpu.VMEM((2, d, HID), BF16),
            pltpu.VMEM((2, HID, d), BF16),
            pltpu.SemaphoreType.DMA((6,)),
            pltpu.SemaphoreType.DMA((2,)),
            pltpu.SemaphoreType.DMA((2,)),
            pltpu.SemaphoreType.DMA((2,)),
        ],
        compiler_params=pltpu.CompilerParams(vmem_limit_bytes=VMEM_BIG),
        cost_estimate=pl.CostEstimate(flops=6 * rows * d * f, bytes_accessed=6 * d * f, transcendentals=0),
        name=name,
    )(*x, *mine, *got, gain, w1, w3, w2, after)


def solution(mesh):
    n_cp = mesh.shape["cp"]
    row_mat = P(("dp", "cp", "tp"), None)
    row_vec = P(("dp", "cp", "tp"))
    col_split = P(None, "tp")
    row_split = P("tp", None)
    swap = [(0, 1), (1, 0)]

    def hop(z, h):
        return lax.ppermute(z, "cp", [(i, i ^ h) for i in range(n_cp)])

    def gather_kv(kv):
        return [kv] + [hop(kv, h) for h in range(1, n_cp)]

    def local_layer(hidden, positions, doc_ids, attn_gain, mlp_gain, wq, wk, wv, wo, w1, w3, w2):
        def swapped(z):
            return lax.ppermute(z, "tp", swap)

        g1, g2 = attn_gain[None, :], mlp_gain[None, :]
        xo1, xo2 = hidden[:PIECE], hidden[PIECE:]
        pos_p = swapped(positions)
        x1 = swapped(xo1)
        x2 = swapped(xo2)
        cos_o, sin_o, po = rope_tables(positions)
        cos_p, sin_p, pp = rope_tables(pos_p)
        c1, s1, c2, s2 = cos_p[:PIECE], sin_p[:PIECE], cos_p[PIECE:], sin_p[PIECE:]
        firsts = jnp.stack([positions[::PIECE], pos_p[::PIECE]])

        kv_o, a_o = kv_call(hidden, g1, cos_o, sin_o, wk, wv, cos_o)
        far_o, near_o = hop(kv_o, 2), hop(kv_o, 1)
        q_o = q_call(a_o, cos_o, sin_o, wq, kv_o)
        kv_1, a_1 = kv_call(x1, g1, c1, s1, wk, wv, q_o)
        all_1 = gather_kv(kv_1)
        q_1 = q_call(a_1, c1, s1, wq, kv_1)
        all_o = [kv_o, near_o, far_o, hop(far_o, 1)]
        early = [z for duo in zip(all_o, all_1) for z in duo]
        m_o1, = attn_call(n_cp, False, ((0, 0),), firsts[0], po, [q_o], wo, q_1, early, "attn_o1")
        got_p1 = swapped(m_o1)
        kv_2, a_2 = kv_call(x2, g1, c2, s2, wk, wv, m_o1)
        all_2 = gather_kv(kv_2)
        q_2 = q_call(a_2, c2, s2, wq, kv_2)
        every = [z for trio in zip(all_o, all_1, all_2) for z in trio]
        m_o2, = attn_call(n_cp, True, ((0, 1),), firsts[0], po, [q_o], wo, q_2, every, "attn_o2")
        got_p2 = swapped(m_o2)
        m_p1, m_p2 = attn_call(n_cp, True, ((1, 0), (1, 1)), firsts[1], pp, [q_1, q_2], wo, m_o2, every, "attn_p")
        got_o1 = swapped(m_p1)
        got_o2 = swapped(m_p2)

        down_p, _ = mlp_call((x1, x2), (m_p1, m_p2), (got_p1, got_p2), g2, w1, w3, w2, m_p2, "mlp_p")
        got_d = swapped(down_p)
        down_o, h_o = mlp_call((xo1, xo2), (m_o1, m_o2), (got_o1, got_o2), g2, w1, w3, w2, down_p, "mlp_o")
        return add_call(h_o, down_o, got_d)

    in_specs = (row_mat, row_vec, row_vec, P(None), P(None), col_split, col_split, col_split, row_split, col_split, col_split, row_split)
    return jax.shard_map(local_layer, mesh=mesh, in_specs=in_specs, out_specs=row_mat, check_vma=False)
```
